16 devices in a mesh: dp: 4 (over z, y), x: 4 (over x, core).
Axes of the slice: x: 2, y: 2, z: 2, core: 2. Of those that a mesh axis runs over, the one named last changes fastest.
Arguments:
- start_pos: int32 [512], P('dp'), parts along dimension 0
- hidden_in: bfloat16 [4, 512, 4096], P(None, ('dp', 'x')), parts along dimension 1
- k_cache: bfloat16 [512, 256, 8, 128], P('dp', None, 'x'), parts along dimension 0
- v_cache: bfloat16 [512, 256, 8, 128], P('dp', None, 'x'), parts along dimension 0
- attn_norm: bfloat16 [4096], replicated
- w_q: bfloat16 [4096, 4096], replicated
- w_k: bfloat16 [4096, 1024], replicated
- w_v: bfloat16 [4096, 1024], replicated
- q_norm: bfloat16 [128], replicated
- k_norm: bfloat16 [128], replicated
- w_o: bfloat16 [4096, 4096], replicated
- mlp_norm: bfloat16 [4096], replicated
- w_gate: bfloat16 [4096, 12288], replicated
- w_up: bfloat16 [4096, 12288], replicated
- w_down: bfloat16 [12288, 4096], replicated
Outputs:
- output 1: bfloat16 [4, 512, 4096], P(None, ('dp', 'x')), parts along dimension 1
- output 2: bfloat16 [512, 256, 8, 128], P(('dp', 'x')), parts along dimension 0
- output 3: bfloat16 [512, 256, 8, 128], P(('dp', 'x')), parts along dimension 0
There are 4 independent parts. The reference program is written for one: setup_inputs(seed, part) draws one part's arguments, and reference() takes and returns one part's arrays. A program takes and returns all parts, laid end to end along the dimension named above; an argument that names none is the same for every part.
All inputs are finite; a program needn't handle non-finite values.
Results may differ from the reference program's by a relative error of at most 0.0104356.
Values are sent between devices in bfloat16 or wider.
A program may use at most 1.75 GiB of HBM per device.

```python
import math
import jax
import jax.numpy as jnp
from jax import lax

BATCH = 128
T = 256
D = 4096
HEADS = 32
KV_HEADS = 8
HEAD = 128
FF = 12288
STEPS = 4

EPS = 1e-6
THETA = 1000000.0
Q_GAIN = math.sqrt(0.8 * math.log(T))
K_GAIN = math.sqrt(2.0 * math.log(T))


def rms_norm(values, gain_vec):
    values32 = values.astype(jnp.float32)
    inv_rms = lax.rsqrt(jnp.mean(values32 * values32, axis=-1, keepdims=True) + EPS)
    return values32 * inv_rms * gain_vec.astype(jnp.float32)


def rotary(values, positions):
    half_dim = HEAD // 2
    inv_freq = jnp.power(THETA, -jnp.arange(half_dim, dtype=jnp.float32) * 2.0 / HEAD)
    angles = positions.astype(jnp.float32)[..., None, None] * inv_freq
    cos_part = jnp.cos(angles)
    sin_part = jnp.sin(angles)
    first_half = values[..., :half_dim]
    second_half = values[..., half_dim:]
    return jnp.concatenate([first_half * cos_part - second_half * sin_part, second_half * cos_part + first_half * sin_part], axis=-1)


def setup_inputs(seed: int = 0, part: int = 0) -> dict:
    base_keys = jax.random.split(jax.random.key(seed), 16)

    def part_normal(index, shape):
        return jax.random.normal(jax.random.fold_in(base_keys[index], part), shape, jnp.float32)

    def shared_normal(index, shape):
        return jax.random.normal(base_keys[index], shape, jnp.float32)

    pos_key = jax.random.fold_in(base_keys[0], part)
    pos_draw = jax.random.randint(jax.random.fold_in(pos_key, 1), (BATCH,), T // 4, T - 3)
    top_row = jax.random.randint(jax.random.fold_in(pos_key, 2), (), 0, BATCH)
    start_pos = jnp.where(jnp.arange(BATCH) == top_row, T - 4, pos_draw).astype(jnp.int32)
    return dict(
        start_pos=start_pos,
        hidden_in=part_normal(1, (STEPS, BATCH, D)).astype(jnp.bfloat16),
        k_cache=part_normal(2, (BATCH, T, KV_HEADS, HEAD)).astype(jnp.bfloat16),
        v_cache=part_normal(3, (BATCH, T, KV_HEADS, HEAD)).astype(jnp.bfloat16),
        attn_norm=(1.0 + 0.2 * shared_normal(4, (D,))).astype(jnp.bfloat16),
        w_q=(shared_normal(5, (D, HEADS * HEAD)) * D ** -0.5).astype(jnp.bfloat16),
        w_k=(shared_normal(6, (D, KV_HEADS * HEAD)) * D ** -0.5).astype(jnp.bfloat16),
        w_v=(shared_normal(7, (D, KV_HEADS * HEAD)) * D ** -0.5).astype(jnp.bfloat16),
        q_norm=(Q_GAIN * (1.0 + 0.2 * shared_normal(8, (HEAD,)))).astype(jnp.bfloat16),
        k_norm=(K_GAIN * (1.0 + 0.2 * shared_normal(9, (HEAD,)))).astype(jnp.bfloat16),
        w_o=(shared_normal(10, (HEADS * HEAD, D)) * (HEADS * HEAD) ** -0.5).astype(jnp.bfloat16),
        mlp_norm=(1.0 + 0.2 * shared_normal(11, (D,))).astype(jnp.bfloat16),
        w_gate=(shared_normal(12, (D, FF)) * D ** -0.5).astype(jnp.bfloat16),
        w_up=(shared_normal(13, (D, FF)) * D ** -0.5).astype(jnp.bfloat16),
        w_down=(shared_normal(14, (FF, D)) * FF ** -0.5).astype(jnp.bfloat16),
    )


def reference(start_pos, hidden_in, k_cache, v_cache, attn_norm, w_q, w_k, w_v, q_norm, k_norm, w_o, mlp_norm, w_gate, w_up, w_down):
    group_size = HEADS // KV_HEADS
    score_scale = HEAD ** -0.5
    tokens = rms_norm(hidden_in, attn_norm).astype(jnp.bfloat16).reshape(STEPS * BATCH, D)
    queries = jnp.dot(tokens, w_q, preferred_element_type=jnp.float32).reshape(STEPS, BATCH, HEADS, HEAD)
    keys_new = jnp.dot(tokens, w_k, preferred_element_type=jnp.float32).reshape(STEPS, BATCH, KV_HEADS, HEAD)
    values_new = jnp.dot(tokens, w_v, preferred_element_type=jnp.float32).reshape(STEPS, BATCH, KV_HEADS, HEAD)
    positions = start_pos[None, :] + jnp.arange(STEPS)[:, None]
    queries = rotary(rms_norm(queries, q_norm), positions).astype(jnp.bfloat16)
    keys_new = rotary(rms_norm(keys_new, k_norm), positions).astype(jnp.bfloat16)
    values_new = values_new.astype(jnp.bfloat16)

    def one_row(row_inputs):
        row_q, row_k, row_v, row_kc, row_vc, row_pos = row_inputs

        def one_step(carry_in, step_inputs):
            cache_k, cache_v = carry_in
            step_q, step_k, step_v, slot_idx = step_inputs
            cache_k = lax.dynamic_update_slice(cache_k, step_k[None], (slot_idx, 0, 0))
            cache_v = lax.dynamic_update_slice(cache_v, step_v[None], (slot_idx, 0, 0))
            grouped = step_q.reshape(KV_HEADS, group_size, HEAD).astype(jnp.float32)
            scores = jnp.einsum('kgd,tkd->kgt', grouped, cache_k.astype(jnp.float32)) * score_scale
            slot_valid = jnp.arange(T) <= slot_idx
            scores = jnp.where(slot_valid, scores, -jnp.inf)
            weights = jnp.exp(scores - jnp.max(scores, axis=-1, keepdims=True))
            weight_sum = jnp.sum(weights, axis=-1)
            mixed_vals = jnp.einsum('kgt,tkd->kgd', weights.astype(jnp.bfloat16).astype(jnp.float32), cache_v.astype(jnp.float32))
            attended = (mixed_vals / weight_sum[..., None]).astype(jnp.bfloat16).reshape(HEADS * HEAD)
            return (cache_k, cache_v), attended

        (final_k, final_v), step_outs = lax.scan(one_step, (row_kc, row_vc), (row_q, row_k, row_v, row_pos + jnp.arange(STEPS)))
        return step_outs, final_k, final_v

    row_outs, k_out, v_out = lax.map(one_row, (jnp.swapaxes(queries, 0, 1), jnp.swapaxes(keys_new, 0, 1), jnp.swapaxes(values_new, 0, 1), k_cache, v_cache, start_pos))
    attended = jnp.swapaxes(row_outs, 0, 1).reshape(STEPS * BATCH, HEADS * HEAD)
    attn_out = jnp.dot(attended, w_o, preferred_element_type=jnp.float32).reshape(STEPS, BATCH, D)
    residual = (hidden_in.astype(jnp.float32) + attn_out).astype(jnp.bfloat16)
    normed = rms_norm(residual, mlp_norm).astype(jnp.bfloat16).reshape(STEPS * BATCH, D)
    gate_val = jnp.dot(normed, w_gate, preferred_element_type=jnp.float32)
    up_val = jnp.dot(normed, w_up, preferred_element_type=jnp.float32)
    activated = (jax.nn.silu(gate_val) * up_val).astype(jnp.bfloat16)
    down_val = jnp.dot(activated, w_down, preferred_element_type=jnp.float32).reshape(STEPS, BATCH, D)
    out_hidden = (residual.astype(jnp.float32) + down_val).astype(jnp.bfloat16)
    return (out_hidden, k_out, v_out)
```

```python
import jax
import jax.numpy as jnp
from jax import lax
from jax.experimental import pallas as pl
from jax.experimental.pallas import tpu as pltpu
from jax.sharding import PartitionSpec as P


EPS = 1e-6
THETA = 1000000.0
GROUP = 4
STEPS = 4
ROWS = 48
BLK = 8
UNITS = ((0, 0, 8), (0, 8, 8), (0, 16, 8), (0, 24, 8), (1, 0, 8), (1, 8, 8), (1, 16, 8), (1, 24, 4), (1, 28, 4))


def rms_norm(values, gain_vec):
    values32 = values.astype(jnp.float32)
    inv_rms = lax.rsqrt(jnp.mean(values32 * values32, axis=-1, keepdims=True) + EPS)
    return values32 * inv_rms * gain_vec.astype(jnp.float32)


def rotary(values, positions):
    head_dim = values.shape[-1]
    half_dim = head_dim // 2
    inv_freq = jnp.power(THETA, -jnp.arange(half_dim, dtype=jnp.float32) * 2.0 / head_dim)
    angles = positions.astype(jnp.float32)[..., None, None] * inv_freq
    cos_part = jnp.cos(angles)
    sin_part = jnp.sin(angles)
    first_half = values[..., :half_dim]
    second_half = values[..., half_dim:]
    return jnp.concatenate([first_half * cos_part - second_half * sin_part, second_half * cos_part + first_half * sin_part], axis=-1)


def project(hidden, positions, attn_norm, w_q, w_k, w_v, q_norm, k_norm):
    n_steps, num_rows = hidden.shape[0], hidden.shape[1]
    head_dim = q_norm.shape[0]
    normed = rms_norm(hidden, attn_norm).astype(jnp.bfloat16)
    queries = jnp.einsum('sbd,de->sbe', normed, w_q, preferred_element_type=jnp.float32).reshape(n_steps, num_rows, -1, head_dim)
    keys_new = jnp.einsum('sbd,de->sbe', normed, w_k, preferred_element_type=jnp.float32).reshape(n_steps, num_rows, -1, head_dim)
    values_new = jnp.einsum('sbd,de->sbe', normed, w_v, preferred_element_type=jnp.float32).reshape(n_steps, num_rows, -1, head_dim)
    queries = rotary(rms_norm(queries, q_norm), positions).astype(jnp.bfloat16)
    keys_new = rotary(rms_norm(keys_new, k_norm), positions).astype(jnp.bfloat16)
    return queries, keys_new, values_new.astype(jnp.bfloat16)


def finish(hidden, flat_attn, w_o, mlp_norm, w_gate, w_up, w_down):
    attn_out = jnp.einsum('sbe,ed->sbd', flat_attn, w_o, preferred_element_type=jnp.float32)
    residual = (hidden.astype(jnp.float32) + attn_out).astype(jnp.bfloat16)
    normed = rms_norm(residual, mlp_norm).astype(jnp.bfloat16)
    gate_val = jnp.einsum('sbd,df->sbf', normed, w_gate, preferred_element_type=jnp.float32)
    up_val = jnp.einsum('sbd,df->sbf', normed, w_up, preferred_element_type=jnp.float32)
    activated = (jax.nn.silu(gate_val) * up_val).astype(jnp.bfloat16)
    down_val = jnp.einsum('sbf,fd->sbd', activated, w_down, preferred_element_type=jnp.float32)
    return (residual.astype(jnp.float32) + down_val).astype(jnp.bfloat16)


def one_sequence(packed, keys, values, pos):
    n_cols = keys.shape[0]
    head_dim = keys.shape[1]
    scale = head_dim ** -0.5
    q = packed[0:32]
    k_new = packed[32:40]
    v_new = packed[40:48]
    nt = (((1,), (1,)), ((), ()))
    old = lax.dot_general(q, keys, nt, preferred_element_type=jnp.float32) * scale
    new = lax.dot_general(q, k_new, nt, preferred_element_type=jnp.float32) * scale
    row = lax.broadcasted_iota(jnp.int32, (32, n_cols), 0)
    col = lax.broadcasted_iota(jnp.int32, (32, n_cols), 1)
    bound = 2 * pos
    ok = jnp.logical_and((col & 1) == (row >> 4), col < bound)
    old = jnp.where(ok, old, -jnp.inf)
    row2 = lax.broadcasted_iota(jnp.int32, (32, 8), 0)
    col2 = lax.broadcasted_iota(jnp.int32, (32, 8), 1)
    ok2 = jnp.logical_and((col2 & 1) == (row2 >> 4), (col2 >> 1) <= (row2 & 3))
    new = jnp.where(ok2, new, -jnp.inf)
    peak = jnp.maximum(jnp.max(old, axis=1, keepdims=True), jnp.max(new, axis=1, keepdims=True))
    w_old = jnp.exp(old - peak)
    w_new = jnp.exp(new - peak)
    total = jnp.sum(w_old, axis=1, keepdims=True) + jnp.sum(w_new, axis=1, keepdims=True)
    mixed = jnp.dot(w_old.astype(jnp.bfloat16), values, preferred_element_type=jnp.float32)
    mixed = mixed + jnp.dot(w_new.astype(jnp.bfloat16), v_new, preferred_element_type=jnp.float32)
    return (mixed / total).astype(jnp.bfloat16)


def attend_source(packed, k_rows, v_rows, start_pos, me):
    n = packed.shape[1]
    seqs = k_rows.shape[0] // GROUP
    per = seqs // BLK

    def body(me_ref, pos_ref, packed_ref, k_ref, v_ref, out_ref):
        base = (me_ref[0] ^ pl.program_id(0)) * seqs + pl.program_id(1) * BLK
        for b in range(BLK):
            out_ref[0, b] = one_sequence(packed_ref[0, b], k_ref[b], v_ref[b], pos_ref[base + b])

    cache_spec = pl.BlockSpec((BLK,) + k_rows.shape[1:], lambda o, i, me_ref, pos_ref: ((me_ref[0] ^ o) * per + i, 0, 0))
    return pl.pallas_call(
        body,
        grid_spec=pltpu.PrefetchScalarGridSpec(
            num_scalar_prefetch=2,
            grid=(GROUP, n // BLK),
            in_specs=[pl.BlockSpec((1, BLK, ROWS, 128), lambda o, i, *_: (o, i, 0, 0)), cache_spec, cache_spec],
            out_specs=pl.BlockSpec((1, BLK, 32, 128), lambda o, i, *_: (o, i, 0, 0)),
        ),
        out_shape=jax.ShapeDtypeStruct((GROUP, n, 32, 128), jnp.bfloat16),
        cost_estimate=pl.CostEstimate(flops=40_000_000_000, bytes_accessed=2 * k_rows.size * 2, transcendentals=0),
        name="attend_source",
    )(me, start_pos, packed, k_rows, v_rows)


def assemble(cache, recvs, fresh, pos, me, first, count, prev):
    seqs = cache.shape[0] // GROUP
    slots = cache.shape[1]
    half = count // 2 if count > 1 else count
    parts = [(p, half) for p in range(0, count, half)]

    def body(me_ref, pos_ref, cache_ref, r1, r2, r3, fresh_ref, *rest):
        out_ref, buf, in_sems, out_sems = rest[-4:]
        mine = me_ref[0]

        def load(p, size, k, off):
            if off == 0:
                src = cache_ref.at[pl.ds(mine * seqs + first + p, size)]
            else:
                src = (r1, r2, r3)[off - 1].at[pl.ds(p, size)]
            return pltpu.make_async_copy(src, buf.at[pl.ds(p, size), :, mine ^ off], in_sems.at[k, off])

        def store(p, size, k):
            return pltpu.make_async_copy(buf.at[pl.ds(p, size)], out_ref.at[pl.ds(first + p, size)], out_sems.at[k])

        for k, (p, size) in enumerate(parts):
            for off in range(GROUP):
                load(p, size, k, off).start()
        for k, (p, size) in enumerate(parts):
            for off in range(GROUP):
                load(p, size, k, off).wait()
            for b in range(size):
                where = pos_ref[first + p + b]
                for s in range(STEPS):
                    buf[p + b, where + s] = fresh_ref[first + p + b, s]
            store(p, size, k).start()
        for k, (p, size) in enumerate(parts):
            store(p, size, k).wait()

    any_spec = pl.BlockSpec(memory_space=pl.ANY)
    smem = pl.BlockSpec(memory_space=pltpu.SMEM)
    args = [me, pos, cache, *recvs, fresh]
    specs = [smem, smem, any_spec, any_spec, any_spec, any_spec, pl.BlockSpec(memory_space=pltpu.VMEM)]
    aliases = {}
    if prev is not None:
        aliases = {len(args): 0}
        args.append(prev)
        specs.append(any_spec)
    return pl.pallas_call(
        body,
        in_specs=specs,
        out_specs=any_spec,
        out_shape=jax.ShapeDtypeStruct((seqs, slots, GROUP, 2, 128), jnp.bfloat16),
        scratch_shapes=[
            pltpu.VMEM((count, slots, GROUP, 2, 128), jnp.bfloat16),
            pltpu.SemaphoreType.DMA((len(parts), GROUP)),
            pltpu.SemaphoreType.DMA((len(parts),)),
        ],
        input_output_aliases=aliases,
        cost_estimate=pl.CostEstimate(flops=count * 1_000_000_000, bytes_accessed=count * slots * 8 * 128 * 4, transcendentals=0),
        name="assemble",
    )(*args)


def solution(mesh):
    row_spec = P(None, ('dp', 'x'), None)
    cache_in = P('dp', None, 'x', None)
    cache_out = P(('dp', 'x'), None, None, None)

    def swap(arr, off):
        return lax.ppermute(arr, 'x', [(i, i ^ off) for i in range(GROUP)])

    def layer(start_pos, hidden_in, k_heads, v_heads, attn_norm, w_q, w_k, w_v, q_norm, k_norm, w_o, mlp_norm, w_gate, w_up, w_down):
        num_rows = hidden_in.shape[1]
        n_steps = hidden_in.shape[0]
        head_dim = q_norm.shape[0]
        slots = k_heads.shape[1]
        me = lax.axis_index('x')
        me_arr = me.reshape(1).astype(jnp.int32)
        my_pos = lax.dynamic_slice_in_dim(start_pos, me * num_rows, num_rows)
        k_rows = k_heads.reshape(k_heads.shape[0], slots * 2, head_dim)
        v_rows = v_heads.reshape(v_heads.shape[0], slots * 2, head_dim)

        def send_unit(u):
            which, first, count = UNITS[u]
            rows = (k_rows, v_rows)[which]
            out = {}
            for off in (2, 3, 1):
                block = lax.dynamic_slice_in_dim(rows, (me ^ off) * num_rows + first, count)
                out[off] = swap(block, off)
            return [out[off].reshape(count, slots, 2, head_dim) for off in (1, 2, 3)]

        recvs = [send_unit(u) for u in range(len(UNITS))]

        positions = my_pos[None, :] + jnp.arange(n_steps)[:, None]
        queries, keys_new, values_new = project(hidden_in, positions, attn_norm, w_q, w_k, w_v, q_norm, k_norm)
        q_pack = queries.reshape(n_steps, num_rows, GROUP, 2, 4, head_dim).transpose(2, 1, 3, 4, 0, 5).reshape(GROUP, num_rows, 32, head_dim)
        kv_shape = (n_steps, num_rows, GROUP, 2, head_dim)
        k_pack = keys_new.reshape(kv_shape).transpose(2, 1, 0, 3, 4).reshape(GROUP, num_rows, 8, head_dim)
        v_pack = values_new.reshape(kv_shape).transpose(2, 1, 0, 3, 4).reshape(GROUP, num_rows, 8, head_dim)
        packed = jnp.concatenate([q_pack, k_pack, v_pack], axis=2)

        def owner_part(arr, off):
            return lax.dynamic_index_in_dim(arr, me ^ off, 0, keepdims=False)

        by_off = [owner_part(packed, 0)] + [swap(owner_part(packed, off), off) for off in (1, 2, 3)]
        mixed = attend_source(jnp.stack(by_off), k_rows, v_rows, start_pos, me_arr)
        back = jnp.stack([mixed[0]] + [swap(mixed[off], off) for off in (1, 2, 3)])
        owners = jnp.stack([owner_part(back, j) for j in range(GROUP)])
        attended = owners.reshape(GROUP, num_rows, 2, 4, n_steps, head_dim).transpose(4, 1, 0, 2, 3, 5).reshape(n_steps, num_rows, -1)
        out_hidden = finish(hidden_in, attended, w_o, mlp_norm, w_gate, w_up, w_down)

        k_fresh = keys_new.reshape(kv_shape).transpose(1, 0, 2, 3, 4)
        v_fresh = values_new.reshape(kv_shape).transpose(1, 0, 2, 3, 4)
        outs = [None, None]
        for u, (which, first, count) in enumerate(UNITS):
            outs[which] = assemble((k_heads, v_heads)[which], recvs[u], (k_fresh, v_fresh)[which], my_pos, me_arr, first, count, outs[which])
        k_out, v_out = outs
        full = (num_rows, slots, 2 * GROUP, head_dim)
        return out_hidden, k_out.reshape(full), v_out.reshape(full)

    return jax.shard_map(layer, mesh=mesh, in_specs=(P('dp'), row_spec, cache_in, cache_in) + (P(),) * 11, out_specs=(row_spec, cache_out, cache_out), check_vma=False)
```

```python
import jax
import jax.numpy as jnp
from jax import lax
from jax.experimental import pallas as pl
from jax.experimental.pallas import tpu as pltpu
from jax.sharding import PartitionSpec as P


EPS = 1e-6
THETA = 1000000.0
GROUP = 4
STEPS = 4
GROUPS = ((0, 2), (2, 8), (10, 6), (16, 2))
EARLY = 18
LATE = ((18, 8), (26, 5), (31, 1))
UNITS = GROUPS + LATE


def rms_norm(values, gain_vec):
    values32 = values.astype(jnp.float32)
    inv_rms = lax.rsqrt(jnp.mean(values32 * values32, axis=-1, keepdims=True) + EPS)
    return values32 * inv_rms * gain_vec.astype(jnp.float32)


def rotary(values, positions):
    head_dim = values.shape[-1]
    half_dim = head_dim // 2
    inv_freq = jnp.power(THETA, -jnp.arange(half_dim, dtype=jnp.float32) * 2.0 / head_dim)
    angles = positions.astype(jnp.float32)[..., None, None] * inv_freq
    cos_part = jnp.cos(angles)
    sin_part = jnp.sin(angles)
    first_half = values[..., :half_dim]
    second_half = values[..., half_dim:]
    return jnp.concatenate([first_half * cos_part - second_half * sin_part, second_half * cos_part + first_half * sin_part], axis=-1)


def project(hidden, positions, attn_norm, w_q, w_k, w_v, q_norm, k_norm):
    n_steps, num_rows = hidden.shape[0], hidden.shape[1]
    head_dim = q_norm.shape[0]
    normed = rms_norm(hidden, attn_norm).astype(jnp.bfloat16)
    queries = jnp.einsum('sbd,de->sbe', normed, w_q, preferred_element_type=jnp.float32).reshape(n_steps, num_rows, -1, head_dim)
    keys_new = jnp.einsum('sbd,de->sbe', normed, w_k, preferred_element_type=jnp.float32).reshape(n_steps, num_rows, -1, head_dim)
    values_new = jnp.einsum('sbd,de->sbe', normed, w_v, preferred_element_type=jnp.float32).reshape(n_steps, num_rows, -1, head_dim)
    queries = rotary(rms_norm(queries, q_norm), positions).astype(jnp.bfloat16)
    keys_new = rotary(rms_norm(keys_new, k_norm), positions).astype(jnp.bfloat16)
    return queries, keys_new, values_new.astype(jnp.bfloat16)


def finish(hidden, flat_attn, w_o, mlp_norm, w_gate, w_up, w_down):
    attn_out = jnp.einsum('sbe,ed->sbd', flat_attn, w_o, preferred_element_type=jnp.float32)
    residual = (hidden.astype(jnp.float32) + attn_out).astype(jnp.bfloat16)
    normed = rms_norm(residual, mlp_norm).astype(jnp.bfloat16)
    gate_val = jnp.einsum('sbd,df->sbf', normed, w_gate, preferred_element_type=jnp.float32)
    up_val = jnp.einsum('sbd,df->sbf', normed, w_up, preferred_element_type=jnp.float32)
    activated = (jax.nn.silu(gate_val) * up_val).astype(jnp.bfloat16)
    down_val = jnp.einsum('sbf,fd->sbd', activated, w_down, preferred_element_type=jnp.float32)
    return (residual.astype(jnp.float32) + down_val).astype(jnp.bfloat16)


def attend_four(packed, keys, values, bounds, own_cols, new_ok):
    scale = keys[0].shape[1] ** -0.5
    nt = (((1,), (1,)), ((), ()))
    items = range(len(keys))
    old = [lax.dot_general(packed[i][0:32], keys[i], nt, preferred_element_type=jnp.float32) for i in items]
    new = [lax.dot_general(packed[i][0:32], packed[i][32:40], nt, preferred_element_type=jnp.float32) for i in items]
    old = [jnp.where(own_cols < bounds[i], old[i] * scale, -jnp.inf) for i in items]
    new = [jnp.where(new_ok, new[i] * scale, -jnp.inf) for i in items]
    peak = [jnp.maximum(jnp.max(old[i], axis=1, keepdims=True), jnp.max(new[i], axis=1, keepdims=True)) for i in items]
    w_old = [jnp.exp(old[i] - peak[i]) for i in items]
    w_new = [jnp.exp(new[i] - peak[i]) for i in items]
    mixed = [jnp.dot(w_old[i].astype(jnp.bfloat16), values[i], preferred_element_type=jnp.float32) for i in items]
    fresh = [jnp.dot(w_new[i].astype(jnp.bfloat16), packed[i][40:48], preferred_element_type=jnp.float32) for i in items]
    total = [jnp.sum(w_old[i], axis=1, keepdims=True) + jnp.sum(w_new[i], axis=1, keepdims=True) for i in items]
    return [((mixed[i] + fresh[i]) / total[i]).astype(jnp.bfloat16) for i in items]


def attend(packed, k_rows, v_rows, recvs, pos, me, first, count):
    seqs = k_rows.shape[0] // GROUP
    rows = k_rows.shape[1]
    here = recvs is not None
    live = rows - 2 * STEPS
    n_in = 5 if here else 2

    def body(me_ref, pos_ref, packed_ref, *rest):
        k_own, v_own = rest[0:2]
        out_ref, k_buf, v_buf, cols, sems = rest[n_in:]
        mine = me_ref[0]

        def load(which, off, b):
            if here and off > 0:
                src = rest[1 + off].at[which, b]
            else:
                src = (k_own, v_own)[which].at[(mine ^ off) * seqs + first + b, pl.ds(0, live)]
            return pltpu.make_async_copy(src, (k_buf, v_buf)[which].at[off, b, pl.ds(0, live)], sems.at[which, off, b])

        @pl.loop(0, count)
        def _(b):
            for off in range(GROUP):
                v_buf[off, b, live:rows] = jnp.zeros((rows - live, 128), jnp.bfloat16)
                load(0, off, b).start()
                load(1, off, b).start()

        row = lax.broadcasted_iota(jnp.int32, (32, rows), 0)
        col = lax.broadcasted_iota(jnp.int32, (32, rows), 1)
        cols[...] = jnp.where((col & 1) == (row >> 4), col, 2 * rows)
        row2 = lax.broadcasted_iota(jnp.int32, (32, 2 * STEPS), 0)
        col2 = lax.broadcasted_iota(jnp.int32, (32, 2 * STEPS), 1)
        new_ok = jnp.logical_and((col2 & 1) == (row2 >> 4), (col2 >> 1) <= (row2 & 3))

        @pl.loop(0, count)
        def _(b):
            for off in range(GROUP):
                load(0, off, b).wait()
                load(1, off, b).wait()
            if here:
                slot = [mine ^ off for off in range(GROUP)]
                items = [packed_ref[slot[off], first + b] for off in range(GROUP)]
                bounds = [2 * pos_ref[first + b]] * GROUP
            else:
                slot = list(range(GROUP))
                items = [packed_ref[off, b] for off in range(GROUP)]
                bounds = [2 * pos_ref[(mine ^ off) * seqs + first + b] for off in range(GROUP)]
            done = attend_four(items, [k_buf[off, b] for off in range(GROUP)], [v_buf[off, b] for off in range(GROUP)], bounds, cols[...], new_ok)
            for off in range(GROUP):
                out_ref[slot[off], b] = done[off]

    any_spec = pl.BlockSpec(memory_space=pl.ANY)
    smem = pl.BlockSpec(memory_space=pltpu.SMEM)
    vmem = pl.BlockSpec(memory_space=pltpu.VMEM)
    return pl.pallas_call(
        body,
        in_specs=[smem, smem, vmem] + [any_spec] * n_in,
        out_specs=vmem,
        out_shape=jax.ShapeDtypeStruct((GROUP, count, 32, 128), jnp.bfloat16),
        scratch_shapes=[
            pltpu.VMEM((GROUP, count, rows, 128), jnp.bfloat16),
            pltpu.VMEM((GROUP, count, rows, 128), jnp.bfloat16),
            pltpu.VMEM((32, rows), jnp.int32),
            pltpu.SemaphoreType.DMA((2, GROUP, count)),
        ],
        cost_estimate=pl.CostEstimate(flops=count * 1_000_000_000, bytes_accessed=4 * count * 512 * 128 * 4, transcendentals=0),
        name="attend_here" if here else "attend_source",
    )(me, pos, packed, k_rows, v_rows, *(recvs or ()))


def spare_slot(where, i, live):
    return jnp.where(where <= live - STEPS, live + i, jnp.minimum(where + STEPS + i, live + STEPS - 1))


def cut(k_heads, v_heads, start_pos, me, first, count):
    seqs = k_heads.shape[0] // GROUP
    slots = k_heads.shape[1]
    live = slots - STEPS
    offs = (2, 3, 1)

    def body(me_ref, pos_ref, k_ref, v_ref, out2, out3, out1, buf, in_sems, out_sems):
        mine = me_ref[0]
        outs = (out2, out3, out1)

        def load(k, c, b):
            return pltpu.make_async_copy((k_ref, v_ref)[c].at[(mine ^ offs[k]) * seqs + first + b], buf.at[k, c, b], in_sems.at[k, c, b])

        def store(k, c, b):
            return pltpu.make_async_copy(buf.at[k, c, b, pl.ds(0, live)], outs[k].at[c, b], out_sems.at[k, c, b])

        for k in range(3):

            @pl.loop(0, count)
            def _(b):
                for c in range(2):
                    load(k, c, b).start()

        for k in range(3):

            @pl.loop(0, count)
            def _(b):
                where = pos_ref[(mine ^ offs[k]) * seqs + first + b]
                for c in range(2):
                    load(k, c, b).wait()
                    for i in range(STEPS):
                        buf[k, c, b, where + i] = buf[k, c, b, spare_slot(where, i, live)]
                    store(k, c, b).start()

        for k in range(3):

            @pl.loop(0, count)
            def _(b):
                for c in range(2):
                    store(k, c, b).wait()

    any_spec = pl.BlockSpec(memory_space=pl.ANY)
    smem = pl.BlockSpec(memory_space=pltpu.SMEM)
    out = pl.pallas_call(
        body,
        in_specs=[smem, smem, any_spec, any_spec],
        out_specs=[any_spec] * 3,
        out_shape=[jax.ShapeDtypeStruct((2, count, live, 2, 128), jnp.bfloat16)] * 3,
        scratch_shapes=[
            pltpu.VMEM((3, 2, count, slots, 2, 128), jnp.bfloat16),
            pltpu.SemaphoreType.DMA((3, 2, count)),
            pltpu.SemaphoreType.DMA((3, 2, count)),
        ],
        cost_estimate=pl.CostEstimate(flops=count * 600_000_000, bytes_accessed=6 * count * slots * 2 * 128 * 4, transcendentals=0),
        name="cut",
    )(me, start_pos, k_heads, v_heads)
    return dict(zip(offs, out))


def assemble(k_heads, v_heads, recvs, fresh, pos, me, first, count, prev):
    seqs = k_heads.shape[0] // GROUP
    slots = k_heads.shape[1]
    live = slots - STEPS

    def body(me_ref, pos_ref, k_ref, v_ref, r1, r2, r3, k_fresh, v_fresh, *rest):
        k_out, v_out, buf, fresh_buf, in_sems, fresh_sems, out_sems = rest[-7:]
        mine = me_ref[0]

        def load(c, b, off):
            if off == 0:
                return pltpu.make_async_copy((k_ref, v_ref)[c].at[mine * seqs + first + b], buf.at[c, b, :, mine], in_sems.at[c, b, 0])
            return pltpu.make_async_copy((r1, r2, r3)[off - 1].at[c, b], buf.at[c, b, pl.ds(0, live), mine ^ off], in_sems.at[c, b, off])

        def load_fresh(c):
            return pltpu.make_async_copy((k_fresh, v_fresh)[c].at[pl.ds(first, count)], fresh_buf.at[c], fresh_sems.at[c])

        def store(c, b):
            return pltpu.make_async_copy(buf.at[c, b], (k_out, v_out)[c].at[first + b], out_sems.at[c, b])

        own = lax.broadcasted_iota(jnp.int32, (GROUP, 2, 128), 0) == mine
        for c in range(2):
            load_fresh(c).start()

        @pl.loop(0, count)
        def _(b):
            for c in range(2):
                for off in range(GROUP):
                    load(c, b, off).start()

        for c in range(2):
            load_fresh(c).wait()

        @pl.loop(0, count)
        def _(b):
            where = pos_ref[first + b]
            for c in range(2):
                for off in range(GROUP):
                    load(c, b, off).wait()
                for i in range(STEPS):
                    spare = spare_slot(where, i, live)
                    moved = jnp.where(own, buf[c, b, spare], buf[c, b, where + i])

                    @pl.when(where + i < live)
                    def _():
                        buf[c, b, spare] = moved

                for s in range(STEPS):
                    buf[c, b, where + s] = fresh_buf[c, b, s]
                store(c, b).start()

        @pl.loop(0, count)
        def _(b):
            for c in range(2):
                store(c, b).wait()

    any_spec = pl.BlockSpec(memory_space=pl.ANY)
    smem = pl.BlockSpec(memory_space=pltpu.SMEM)
    args = [me, pos, k_heads, v_heads, *recvs, *fresh]
    aliases = {}
    if prev is not None:
        aliases = {len(args): 0, len(args) + 1: 1}
        args += prev
    return pl.pallas_call(
        body,
        in_specs=[smem, smem] + [any_spec] * (len(args) - 2),
        out_specs=[any_spec] * 2,
        out_shape=[jax.ShapeDtypeStruct((seqs, slots, GROUP, 2, 128), jnp.bfloat16)] * 2,
        scratch_shapes=[
            pltpu.VMEM((2, count, slots, GROUP, 2, 128), jnp.bfloat16),
            pltpu.VMEM((2, count, STEPS, GROUP, 2, 128), jnp.bfloat16),
            pltpu.SemaphoreType.DMA((2, count, GROUP)),
            pltpu.SemaphoreType.DMA((2,)),
            pltpu.SemaphoreType.DMA((2, count)),
        ],
        input_output_aliases=aliases,
        cost_estimate=pl.CostEstimate(flops=count * 600_000_000, bytes_accessed=2 * count * slots * 8 * 128 * 4, transcendentals=0),
        name="assemble",
    )(*args)


def solution(mesh):
    row_spec = P(None, ('dp', 'x'), None)
    cache_in = P('dp', None, 'x', None)
    cache_out = P(('dp', 'x'), None, None, None)

    def swap(arr, off):
        return lax.ppermute(arr, 'x', [(i, i ^ off) for i in range(GROUP)])

    def layer(start_pos, hidden_in, k_heads, v_heads, attn_norm, w_q, w_k, w_v, q_norm, k_norm, w_o, mlp_norm, w_gate, w_up, w_down):
        num_rows = hidden_in.shape[1]
        n_steps = hidden_in.shape[0]
        head_dim = q_norm.shape[0]
        slots = k_heads.shape[1]
        me = lax.axis_index('x')
        me_arr = me.reshape(1).astype(jnp.int32)
        my_pos = lax.dynamic_slice_in_dim(start_pos, me * num_rows, num_rows)
        k_rows = k_heads.reshape(k_heads.shape[0], slots * 2, head_dim)
        v_rows = v_heads.reshape(v_heads.shape[0], slots * 2, head_dim)

        def send_unit(u):
            first, count = UNITS[u]
            parts = cut(k_heads, v_heads, start_pos, me_arr, first, count)
            out = {off: swap(parts[off], off) for off in (2, 3, 1)}
            return [out[off] for off in (1, 2, 3)]

        recvs = [send_unit(u) for u in range(len(UNITS))]

        positions = my_pos[None, :] + jnp.arange(n_steps)[:, None]
        queries, keys_new, values_new = project(hidden_in, positions, attn_norm, w_q, w_k, w_v, q_norm, k_norm)
        q_pack = queries.reshape(n_steps, num_rows, GROUP, 2, 4, head_dim).transpose(2, 1, 3, 4, 0, 5).reshape(GROUP, num_rows, 32, head_dim)
        kv_shape = (n_steps, num_rows, GROUP, 2, head_dim)
        k_pack = keys_new.reshape(kv_shape).transpose(2, 1, 0, 3, 4).reshape(GROUP, num_rows, 8, head_dim)
        v_pack = values_new.reshape(kv_shape).transpose(2, 1, 0, 3, 4).reshape(GROUP, num_rows, 8, head_dim)
        packed = jnp.concatenate([q_pack, k_pack, v_pack], axis=2)

        def owner_part(arr, off):
            return lax.dynamic_index_in_dim(arr, me ^ off, 0, keepdims=False)

        late = packed[:, EARLY:]
        by_off = [owner_part(late, 0)] + [swap(owner_part(late, off), off) for off in (1, 2, 3)]
        mixed = attend(jnp.stack(by_off), k_rows, v_rows, None, start_pos, me_arr, EARLY, num_rows - EARLY)
        back = jnp.stack([mixed[0]] + [swap(mixed[off], off) for off in (1, 2, 3)])
        here = []
        for g, (first, count) in enumerate(GROUPS):
            arrived = [r.reshape(2, count, -1, head_dim) for r in recvs[g]]
            here.append(attend(packed, k_rows, v_rows, arrived, my_pos, me_arr, first, count))
        there = jnp.stack([owner_part(back, j) for j in range(GROUP)])
        owners = jnp.concatenate(here + [there], axis=1)
        attended = owners.reshape(GROUP, num_rows, 2, 4, n_steps, head_dim).transpose(4, 1, 0, 2, 3, 5).reshape(n_steps, num_rows, -1)
        out_hidden = finish(hidden_in, attended, w_o, mlp_norm, w_gate, w_up, w_down)

        k_fresh = keys_new.reshape(kv_shape).transpose(1, 0, 2, 3, 4)
        v_fresh = values_new.reshape(kv_shape).transpose(1, 0, 2, 3, 4)
        outs = None
        for u, (first, count) in enumerate(UNITS):
            outs = assemble(k_heads, v_heads, recvs[u], (k_fresh, v_fresh), my_pos, me_arr, first, count, outs)
        k_out, v_out = outs
        full = (num_rows, slots, 2 * GROUP, head_dim)
        return out_hidden, k_out.reshape(full), v_out.reshape(full)


    return jax.shard_map(layer, mesh=mesh, in_specs=(P('dp'), row_spec, cache_in, cache_in) + (P(),) * 11, out_specs=(row_spec, cache_out, cache_out), check_vma=False)
```

```python
import jax
import jax.numpy as jnp
from jax import lax
from jax.experimental import pallas as pl
from jax.experimental.pallas import tpu as pltpu
from jax.sharding import PartitionSpec as P


EPS = 1e-6
THETA = 1000000.0
GROUP = 4
STEPS = 4
GROUPS = ((0, 2), (2, 4), (6, 4), (10, 6), (16, 3))
EARLY = 19
LATE = ((19, 8), (27, 4), (31, 1))
UNITS = GROUPS + LATE
ASSEMBLIES = ((0, 1), (2,), (3,), (4, 5), (6,), (7,))


def rms_norm(values, gain_vec):
    values32 = values.astype(jnp.float32)
    inv_rms = lax.rsqrt(jnp.mean(values32 * values32, axis=-1, keepdims=True) + EPS)
    return values32 * inv_rms * gain_vec.astype(jnp.float32)


def rotary(values, positions):
    head_dim = values.shape[-1]
    half_dim = head_dim // 2
    inv_freq = jnp.power(THETA, -jnp.arange(half_dim, dtype=jnp.float32) * 2.0 / head_dim)
    angles = positions.astype(jnp.float32)[..., None, None] * inv_freq
    cos_part = jnp.cos(angles)
    sin_part = jnp.sin(angles)
    first_half = values[..., :half_dim]
    second_half = values[..., half_dim:]
    return jnp.concatenate([first_half * cos_part - second_half * sin_part, second_half * cos_part + first_half * sin_part], axis=-1)


def project(hidden, positions, attn_norm, w_q, w_k, w_v, q_norm, k_norm):
    n_steps, num_rows = hidden.shape[0], hidden.shape[1]
    head_dim = q_norm.shape[0]
    normed = rms_norm(hidden, attn_norm).astype(jnp.bfloat16)
    queries = jnp.einsum('sbd,de->sbe', normed, w_q, preferred_element_type=jnp.float32).reshape(n_steps, num_rows, -1, head_dim)
    keys_new = jnp.einsum('sbd,de->sbe', normed, w_k, preferred_element_type=jnp.float32).reshape(n_steps, num_rows, -1, head_dim)
    values_new = jnp.einsum('sbd,de->sbe', normed, w_v, preferred_element_type=jnp.float32).reshape(n_steps, num_rows, -1, head_dim)
    queries = rotary(rms_norm(queries, q_norm), positions).astype(jnp.bfloat16)
    keys_new = rotary(rms_norm(keys_new, k_norm), positions).astype(jnp.bfloat16)
    return queries, keys_new, values_new.astype(jnp.bfloat16)


def finish(hidden, flat_attn, w_o, mlp_norm, w_gate, w_up, w_down):
    attn_out = jnp.einsum('sbe,ed->sbd', flat_attn, w_o, preferred_element_type=jnp.float32)
    residual = (hidden.astype(jnp.float32) + attn_out).astype(jnp.bfloat16)
    normed = rms_norm(residual, mlp_norm).astype(jnp.bfloat16)
    gate_val = jnp.einsum('sbd,df->sbf', normed, w_gate, preferred_element_type=jnp.float32)
    up_val = jnp.einsum('sbd,df->sbf', normed, w_up, preferred_element_type=jnp.float32)
    activated = (jax.nn.silu(gate_val) * up_val).astype(jnp.bfloat16)
    down_val = jnp.einsum('sbf,fd->sbd', activated, w_down, preferred_element_type=jnp.float32)
    return (residual.astype(jnp.float32) + down_val).astype(jnp.bfloat16)


def attend_four(packed, keys, values, bounds, own_cols, new_ok):
    scale = keys[0].shape[1] ** -0.5
    nt = (((1,), (1,)), ((), ()))
    items = range(len(keys))
    old = [lax.dot_general(packed[i][0:32], keys[i], nt, preferred_element_type=jnp.float32) for i in items]
    new = [lax.dot_general(packed[i][0:32], packed[i][32:40], nt, preferred_element_type=jnp.float32) for i in items]
    old = [jnp.where(own_cols < bounds[i], old[i] * scale, -jnp.inf) for i in items]
    new = [jnp.where(new_ok, new[i] * scale, -jnp.inf) for i in items]
    peak = [jnp.maximum(jnp.max(old[i], axis=1, keepdims=True), jnp.max(new[i], axis=1, keepdims=True)) for i in items]
    w_old = [jnp.exp(old[i] - peak[i]) for i in items]
    w_new = [jnp.exp(new[i] - peak[i]) for i in items]
    mixed = [jnp.dot(w_old[i].astype(jnp.bfloat16), values[i], preferred_element_type=jnp.float32) for i in items]
    fresh = [jnp.dot(w_new[i].astype(jnp.bfloat16), packed[i][40:48], preferred_element_type=jnp.float32) for i in items]
    total = [jnp.sum(w_old[i], axis=1, keepdims=True) + jnp.sum(w_new[i], axis=1, keepdims=True) for i in items]
    return [((mixed[i] + fresh[i]) / total[i]).astype(jnp.bfloat16) for i in items]


def attend(packed, k_rows, v_rows, recvs, pos, me, first, count):
    seqs = k_rows.shape[0] // GROUP
    rows = k_rows.shape[1]
    here = recvs is not None
    live = recvs[0].shape[2] if here else rows - 2 * STEPS
    n_in = 5 if here else 2

    def body(me_ref, pos_ref, packed_ref, *rest):
        k_own, v_own = rest[0:2]
        out_ref, k_buf, v_buf, cols, sems = rest[n_in:]
        mine = me_ref[0]

        def load(which, off, b):
            if here and off > 0:
                src = rest[1 + off].at[which, b]
            else:
                src = (k_own, v_own)[which].at[(mine ^ off) * seqs + first + b, pl.ds(0, live)]
            return pltpu.make_async_copy(src, (k_buf, v_buf)[which].at[off, b, pl.ds(0, live)], sems.at[which, off, b])

        @pl.loop(0, count)
        def _(b):
            for off in range(GROUP):
                if live < rows:
                    v_buf[off, b, live:rows] = jnp.zeros((rows - live, 128), jnp.bfloat16)
                load(0, off, b).start()
                load(1, off, b).start()

        row = lax.broadcasted_iota(jnp.int32, (32, rows), 0)
        col = lax.broadcasted_iota(jnp.int32, (32, rows), 1)
        cols[...] = jnp.where((col & 1) == (row >> 4), col, 2 * rows)
        row2 = lax.broadcasted_iota(jnp.int32, (32, 2 * STEPS), 0)
        col2 = lax.broadcasted_iota(jnp.int32, (32, 2 * STEPS), 1)
        new_ok = jnp.logical_and((col2 & 1) == (row2 >> 4), (col2 >> 1) <= (row2 & 3))

        @pl.loop(0, count)
        def _(b):
            for off in range(GROUP):
                load(0, off, b).wait()
                load(1, off, b).wait()
            if here:
                slot = [mine ^ off for off in range(GROUP)]
                items = [packed_ref[slot[off], first + b] for off in range(GROUP)]
                bounds = [2 * pos_ref[first + b]] * GROUP
            else:
                slot = list(range(GROUP))
                items = [packed_ref[off, b] for off in range(GROUP)]
                bounds = [2 * pos_ref[(mine ^ off) * seqs + first + b] for off in range(GROUP)]
            done = attend_four(items, [k_buf[off, b] for off in range(GROUP)], [v_buf[off, b] for off in range(GROUP)], bounds, cols[...], new_ok)
            for off in range(GROUP):
                out_ref[slot[off], b] = done[off]

    any_spec = pl.BlockSpec(memory_space=pl.ANY)
    smem = pl.BlockSpec(memory_space=pltpu.SMEM)
    vmem = pl.BlockSpec(memory_space=pltpu.VMEM)
    return pl.pallas_call(
        body,
        in_specs=[smem, smem, vmem] + [any_spec] * n_in,
        out_specs=vmem,
        out_shape=jax.ShapeDtypeStruct((GROUP, count, 32, 128), jnp.bfloat16),
        scratch_shapes=[
            pltpu.VMEM((GROUP, count, rows, 128), jnp.bfloat16),
            pltpu.VMEM((GROUP, count, rows, 128), jnp.bfloat16),
            pltpu.VMEM((32, rows), jnp.int32),
            pltpu.SemaphoreType.DMA((2, GROUP, count)),
        ],
        cost_estimate=pl.CostEstimate(flops=count * 1_000_000_000, bytes_accessed=4 * count * 512 * 128 * 4, transcendentals=0),
        name="attend_here" if here else "attend_source",
    )(me, pos, packed, k_rows, v_rows, *(recvs or ()))


def spare_slot(where, i, live):
    return jnp.where(where <= live - STEPS, live + i, jnp.minimum(where + STEPS + i, live + STEPS - 1))


def cut(k_heads, v_heads, start_pos, me, first, count):
    seqs = k_heads.shape[0] // GROUP
    slots = k_heads.shape[1]
    live = slots - STEPS
    offs = (2, 3, 1)

    def body(me_ref, pos_ref, k_ref, v_ref, out2, out3, out1, buf, in_sems, out_sems):
        mine = me_ref[0]
        outs = (out2, out3, out1)

        def load(k, c, b):
            return pltpu.make_async_copy((k_ref, v_ref)[c].at[(mine ^ offs[k]) * seqs + first + b], buf.at[k, c, b], in_sems.at[k, c, b])

        def store(k, c, b):
            return pltpu.make_async_copy(buf.at[k, c, b, pl.ds(0, live)], outs[k].at[c, b], out_sems.at[k, c, b])

        for k in range(3):

            @pl.loop(0, count)
            def _(b):
                for c in range(2):
                    load(k, c, b).start()

        for k in range(3):

            @pl.loop(0, count)
            def _(b):
                where = pos_ref[(mine ^ offs[k]) * seqs + first + b]
                for c in range(2):
                    load(k, c, b).wait()
                    for i in range(STEPS):
                        buf[k, c, b, where + i] = buf[k, c, b, spare_slot(where, i, live)]
                    store(k, c, b).start()

        for k in range(3):

            @pl.loop(0, count)
            def _(b):
                for c in range(2):
                    store(k, c, b).wait()

    any_spec = pl.BlockSpec(memory_space=pl.ANY)
    smem = pl.BlockSpec(memory_space=pltpu.SMEM)
    out = pl.pallas_call(
        body,
        in_specs=[smem, smem, any_spec, any_spec],
        out_specs=[any_spec] * 3,
        out_shape=[jax.ShapeDtypeStruct((2, count, live, 2, 128), jnp.bfloat16)] * 3,
        scratch_shapes=[
            pltpu.VMEM((3, 2, count, slots, 2, 128), jnp.bfloat16),
            pltpu.SemaphoreType.DMA((3, 2, count)),
            pltpu.SemaphoreType.DMA((3, 2, count)),
        ],
        cost_estimate=pl.CostEstimate(flops=count * 600_000_000, bytes_accessed=6 * count * slots * 2 * 128 * 4, transcendentals=0),
        name="cut",
    )(me, start_pos, k_heads, v_heads)
    return dict(zip(offs, out))


def assemble(k_heads, v_heads, units, fresh, pos, me, prev):
    seqs = k_heads.shape[0] // GROUP
    slots = k_heads.shape[1]
    total = sum(count for _, count, _ in units)
    starts = [sum(count for _, count, _ in units[:u]) for u in range(len(units))]

    def body(me_ref, pos_ref, k_ref, v_ref, k_fresh, v_fresh, *rest):
        k_out, v_out, buf, fresh_buf, in_sems, fresh_sems, out_sems = rest[-7:]
        mine = me_ref[0]

        def load(u, c, b, off):
            at = starts[u] + b
            live = units[u][2][0].shape[2]
            if off == 0:
                src = (k_ref, v_ref)[c].at[mine * seqs + units[u][0] + b]
                return pltpu.make_async_copy(src, buf.at[c, at, :, mine], in_sems.at[c, at, 0])
            return pltpu.make_async_copy(rest[3 * u + off - 1].at[c, b], buf.at[c, at, pl.ds(0, live), mine ^ off], in_sems.at[c, at, off])

        def load_fresh(u, c):
            first, count, _ = units[u]
            return pltpu.make_async_copy((k_fresh, v_fresh)[c].at[pl.ds(first, count)], fresh_buf.at[c, pl.ds(starts[u], count)], fresh_sems.at[u, c])

        def store(u, c, b):
            at = starts[u] + b
            return pltpu.make_async_copy(buf.at[c, at], (k_out, v_out)[c].at[units[u][0] + b], out_sems.at[c, at])

        own = lax.broadcasted_iota(jnp.int32, (GROUP, 2, 128), 0) == mine
        for u in range(len(units)):
            for c in range(2):
                load_fresh(u, c).start()

        for u, (_, count, _) in enumerate(units):

            @pl.loop(0, count)
            def _(b):
                for c in range(2):
                    for off in range(GROUP):
                        load(u, c, b, off).start()

        for u, (first, count, recvs) in enumerate(units):
            live = recvs[0].shape[2]
            for c in range(2):
                load_fresh(u, c).wait()

            @pl.loop(0, count)
            def _(b):
                at = starts[u] + b
                where = pos_ref[first + b]
                for c in range(2):
                    for off in range(GROUP):
                        load(u, c, b, off).wait()
                    for i in range(STEPS if live < slots else 0):
                        spare = spare_slot(where, i, live)
                        moved = jnp.where(own, buf[c, at, spare], buf[c, at, where + i])

                        @pl.when(where + i < live)
                        def _():
                            buf[c, at, spare] = moved

                    for s in range(STEPS):
                        buf[c, at, where + s] = fresh_buf[c, at, s]
                    store(u, c, b).start()

        for u, (_, count, _) in enumerate(units):

            @pl.loop(0, count)
            def _(b):
                for c in range(2):
                    store(u, c, b).wait()

    any_spec = pl.BlockSpec(memory_space=pl.ANY)
    smem = pl.BlockSpec(memory_space=pltpu.SMEM)
    args = [me, pos, k_heads, v_heads, *fresh]
    for _, _, recvs in units:
        args += recvs
    aliases = {}
    if prev is not None:
        aliases = {len(args): 0, len(args) + 1: 1}
        args += prev
    return pl.pallas_call(
        body,
        in_specs=[smem, smem] + [any_spec] * (len(args) - 2),
        out_specs=[any_spec] * 2,
        out_shape=[jax.ShapeDtypeStruct((seqs, slots, GROUP, 2, 128), jnp.bfloat16)] * 2,
        scratch_shapes=[
            pltpu.VMEM((2, total, slots, GROUP, 2, 128), jnp.bfloat16),
            pltpu.VMEM((2, total, STEPS, GROUP, 2, 128), jnp.bfloat16),
            pltpu.SemaphoreType.DMA((2, total, GROUP)),
            pltpu.SemaphoreType.DMA((len(units), 2)),
            pltpu.SemaphoreType.DMA((2, total)),
        ],
        input_output_aliases=aliases,
        cost_estimate=pl.CostEstimate(flops=total * 600_000_000, bytes_accessed=2 * total * slots * 8 * 128 * 4, transcendentals=0),
        name="assemble",
    )(*args)


def solution(mesh):
    row_spec = P(None, ('dp', 'x'), None)
    cache_in = P('dp', None, 'x', None)
    cache_out = P(('dp', 'x'), None, None, None)

    def swap(arr, off):
        return lax.ppermute(arr, 'x', [(i, i ^ off) for i in range(GROUP)])

    def layer(start_pos, hidden_in, k_heads, v_heads, attn_norm, w_q, w_k, w_v, q_norm, k_norm, w_o, mlp_norm, w_gate, w_up, w_down):
        num_rows = hidden_in.shape[1]
        n_steps = hidden_in.shape[0]
        head_dim = q_norm.shape[0]
        slots = k_heads.shape[1]
        me = lax.axis_index('x')
        me_arr = me.reshape(1).astype(jnp.int32)
        my_pos = lax.dynamic_slice_in_dim(start_pos, me * num_rows, num_rows)
        k_rows = k_heads.reshape(k_heads.shape[0], slots * 2, head_dim)
        v_rows = v_heads.reshape(v_heads.shape[0], slots * 2, head_dim)

        def send_unit(u):
            first, count = UNITS[u]
            if u == 0:
                out = {}
                for off in (2, 3, 1):
                    at = ((me ^ off) * num_rows + first, 0, 0)
                    both = [swap(lax.dynamic_slice(rows, at, (count,) + rows.shape[1:]), off) for rows in (k_rows, v_rows)]
                    out[off] = both
            else:
                parts = cut(k_heads, v_heads, start_pos, me_arr, first, count)
                out = {off: swap(parts[off], off) for off in (2, 3, 1)}
            if u == 0:
                out = {off: jnp.stack(both).reshape(2, count, slots, 2, head_dim) for off, both in out.items()}
            return [out[off] for off in (1, 2, 3)]

        recvs = [send_unit(u) for u in range(len(UNITS))]

        positions = my_pos[None, :] + jnp.arange(n_steps)[:, None]
        queries, keys_new, values_new = project(hidden_in, positions, attn_norm, w_q, w_k, w_v, q_norm, k_norm)
        q_pack = queries.reshape(n_steps, num_rows, GROUP, 2, 4, head_dim).transpose(2, 1, 3, 4, 0, 5).reshape(GROUP, num_rows, 32, head_dim)
        kv_shape = (n_steps, num_rows, GROUP, 2, head_dim)
        k_pack = keys_new.reshape(kv_shape).transpose(2, 1, 0, 3, 4).reshape(GROUP, num_rows, 8, head_dim)
        v_pack = values_new.reshape(kv_shape).transpose(2, 1, 0, 3, 4).reshape(GROUP, num_rows, 8, head_dim)
        packed = jnp.concatenate([q_pack, k_pack, v_pack], axis=2)

        def owner_part(arr, off):
            return lax.dynamic_index_in_dim(arr, me ^ off, 0, keepdims=False)

        late = packed[:, EARLY:]
        by_off = [owner_part(late, 0)] + [swap(owner_part(late, off), off) for off in (1, 2, 3)]
        mixed = attend(jnp.stack(by_off), k_rows, v_rows, None, start_pos, me_arr, EARLY, num_rows - EARLY)
        back = jnp.stack([mixed[0]] + [swap(mixed[off], off) for off in (1, 2, 3)])
        here = []
        for g, (first, count) in enumerate(GROUPS):
            arrived = [r.reshape(2, count, -1, head_dim) for r in recvs[g]]
            here.append(attend(packed, k_rows, v_rows, arrived, my_pos, me_arr, first, count))
        there = jnp.stack([owner_part(back, j) for j in range(GROUP)])
        owners = jnp.concatenate(here + [there], axis=1)
        attended = owners.reshape(GROUP, num_rows, 2, 4, n_steps, head_dim).transpose(4, 1, 0, 2, 3, 5).reshape(n_steps, num_rows, -1)
        out_hidden = finish(hidden_in, attended, w_o, mlp_norm, w_gate, w_up, w_down)

        k_fresh = keys_new.reshape(kv_shape).transpose(1, 0, 2, 3, 4)
        v_fresh = values_new.reshape(kv_shape).transpose(1, 0, 2, 3, 4)
        outs = None
        for some in ASSEMBLIES:
            outs = assemble(k_heads, v_heads, [(*UNITS[u], recvs[u]) for u in some], (k_fresh, v_fresh), my_pos, me_arr, outs)
        k_out, v_out = outs
        full = (num_rows, slots, 2 * GROUP, head_dim)
        return out_hidden, k_out.reshape(full), v_out.reshape(full)


    return jax.shard_map(layer, mesh=mesh, in_specs=(P('dp'), row_spec, cache_in, cache_in) + (P(),) * 11, out_specs=(row_spec, cache_out, cache_out), check_vma=False)
```

```python
import jax
import jax.numpy as jnp
from jax import lax
from jax.experimental import pallas as pl
from jax.experimental.pallas import tpu as pltpu
from jax.sharding import PartitionSpec as P


EPS = 1e-6
THETA = 1000000.0
GROUP = 4
STEPS = 4
GROUPS = ((0, 2), (2, 8), (10, 9), (19, 3))
EARLY = 22
LATE = ((22, 6), (28, 3), (31, 1))
UNITS = GROUPS + LATE
ASSEMBLIES = ((0, 1), (2,), (3, 4), (5,), (6,))


def rms_norm(values, gain_vec):
    values32 = values.astype(jnp.float32)
    inv_rms = lax.rsqrt(jnp.mean(values32 * values32, axis=-1, keepdims=True) + EPS)
    return values32 * inv_rms * gain_vec.astype(jnp.float32)


def rotary(values, positions):
    head_dim = values.shape[-1]
    half_dim = head_dim // 2
    inv_freq = jnp.power(THETA, -jnp.arange(half_dim, dtype=jnp.float32) * 2.0 / head_dim)
    angles = positions.astype(jnp.float32)[..., None, None] * inv_freq
    cos_part = jnp.cos(angles)
    sin_part = jnp.sin(angles)
    first_half = values[..., :half_dim]
    second_half = values[..., half_dim:]
    return jnp.concatenate([first_half * cos_part - second_half * sin_part, second_half * cos_part + first_half * sin_part], axis=-1)


def project(hidden, positions, attn_norm, w_q, w_k, w_v, q_norm, k_norm):
    n_steps, num_rows = hidden.shape[0], hidden.shape[1]
    head_dim = q_norm.shape[0]
    normed = rms_norm(hidden, attn_norm).astype(jnp.bfloat16)
    queries = jnp.einsum('sbd,de->sbe', normed, w_q, preferred_element_type=jnp.float32).reshape(n_steps, num_rows, -1, head_dim)
    keys_new = jnp.einsum('sbd,de->sbe', normed, w_k, preferred_element_type=jnp.float32).reshape(n_steps, num_rows, -1, head_dim)
    values_new = jnp.einsum('sbd,de->sbe', normed, w_v, preferred_element_type=jnp.float32).reshape(n_steps, num_rows, -1, head_dim)
    queries = rotary(rms_norm(queries, q_norm), positions).astype(jnp.bfloat16)
    keys_new = rotary(rms_norm(keys_new, k_norm), positions).astype(jnp.bfloat16)
    return queries, keys_new, values_new.astype(jnp.bfloat16)


def gated_mlp(rows, w_gate, w_up, w_down, core):
    n, d = rows.shape[1:]
    ff = w_gate.shape[1]
    blk = 512
    steps = ff // 2 // blk

    def body(core_ref, rows_ref, gate_ref, up_ref, down_ref, mine_ref, other_ref, acc_ref):
        x = rows_ref[...].reshape(2 * n, d)
        gate_val = jnp.dot(x, gate_ref[...], preferred_element_type=jnp.float32)
        up_val = jnp.dot(x, up_ref[...], preferred_element_type=jnp.float32)
        activated = (gate_val * jax.nn.sigmoid(gate_val) * up_val).astype(jnp.bfloat16)
        part = jnp.dot(activated, down_ref[...], preferred_element_type=jnp.float32)

        @pl.when(pl.program_id(0) == 0)
        def _():
            acc_ref[...] = part

        @pl.when(pl.program_id(0) > 0)
        def _():
            acc_ref[...] += part

        @pl.when(pl.program_id(0) == steps - 1)
        def _():
            mine_ref[...] = acc_ref[0:n]
            other_ref[...] = acc_ref[n:2 * n]

    column = pl.BlockSpec((d, blk), lambda j, core_ref: (0, core_ref[0] * steps + j))
    whole = pl.BlockSpec((n, d), lambda j, core_ref: (0, 0))
    return pl.pallas_call(
        body,
        grid_spec=pltpu.PrefetchScalarGridSpec(
            num_scalar_prefetch=1,
            grid=(steps,),
            in_specs=[
                pl.BlockSpec((2, n, d), lambda j, core_ref: (0, 0, 0)),
                column,
                column,
                pl.BlockSpec((blk, d), lambda j, core_ref: (core_ref[0] * steps + j, 0)),
            ],
            out_specs=[whole, whole],
            scratch_shapes=[pltpu.VMEM((2 * n, d), jnp.float32)],
        ),
        out_shape=[jax.ShapeDtypeStruct((n, d), jnp.float32)] * 2,
        compiler_params=pltpu.CompilerParams(vmem_limit_bytes=62 * 1024 * 1024),
        cost_estimate=pl.CostEstimate(flops=6 * n * d * ff, bytes_accessed=3 * d * ff, transcendentals=n * ff),
        name="gated_mlp",
    )(core, rows, w_gate, w_up, w_down)


def finish(hidden, flat_attn, w_o, mlp_norm, w_gate, w_up, w_down, core, swap_core):
    attn_out = jnp.einsum('sbe,ed->sbd', flat_attn, w_o, preferred_element_type=jnp.float32)
    residual = (hidden.astype(jnp.float32) + attn_out).astype(jnp.bfloat16)
    normed = rms_norm(residual, mlp_norm).astype(jnp.bfloat16)
    flat = normed.reshape(-1, normed.shape[-1])
    mine, other = gated_mlp(jnp.stack([flat, swap_core(flat)]), w_gate, w_up, w_down, core)
    down_val = mine + swap_core(other)
    return (residual.astype(jnp.float32) + down_val.reshape(residual.shape)).astype(jnp.bfloat16)


def attend_four(packed, keys, values, bounds, own_cols, new_ok):
    scale = keys[0].shape[1] ** -0.5
    nt = (((1,), (1,)), ((), ()))
    items = range(len(keys))
    old = [lax.dot_general(packed[i][0:32], keys[i], nt, preferred_element_type=jnp.float32) for i in items]
    new = [lax.dot_general(packed[i][0:32], packed[i][32:40], nt, preferred_element_type=jnp.float32) for i in items]
    old = [jnp.where(own_cols < bounds[i], old[i] * scale, -jnp.inf) for i in items]
    new = [jnp.where(new_ok, new[i] * scale, -jnp.inf) for i in items]
    peak = [jnp.maximum(jnp.max(old[i], axis=1, keepdims=True), jnp.max(new[i], axis=1, keepdims=True)) for i in items]
    w_old = [jnp.exp(old[i] - peak[i]) for i in items]
    w_new = [jnp.exp(new[i] - peak[i]) for i in items]
    mixed = [jnp.dot(w_old[i].astype(jnp.bfloat16), values[i], preferred_element_type=jnp.float32) for i in items]
    fresh = [jnp.dot(w_new[i].astype(jnp.bfloat16), packed[i][40:48], preferred_element_type=jnp.float32) for i in items]
    total = [jnp.sum(w_old[i], axis=1, keepdims=True) + jnp.sum(w_new[i], axis=1, keepdims=True) for i in items]
    return [((mixed[i] + fresh[i]) / total[i]).astype(jnp.bfloat16) for i in items]


def attend(packed, k_rows, v_rows, recvs, pos, me, first, count):
    seqs = k_rows.shape[0] // GROUP
    rows = k_rows.shape[1]
    here = recvs is not None
    live = recvs[0].shape[2] if here else rows - 2 * STEPS
    n_in = 5 if here else 2

    def body(me_ref, pos_ref, packed_ref, *rest):
        k_own, v_own = rest[0:2]
        out_ref, k_buf, v_buf, cols, sems = rest[n_in:]
        mine = me_ref[0]

        def load(which, off, b):
            if here and off > 0:
                src = rest[1 + off].at[which, b]
            else:
                src = (k_own, v_own)[which].at[(mine ^ off) * seqs + first + b, pl.ds(0, live)]
            return pltpu.make_async_copy(src, (k_buf, v_buf)[which].at[off, b, pl.ds(0, live)], sems.at[which, off, b])

        @pl.loop(0, count)
        def _(b):
            for off in range(GROUP):
                if live < rows:
                    v_buf[off, b, live:rows] = jnp.zeros((rows - live, 128), jnp.bfloat16)
                load(0, off, b).start()
                load(1, off, b).start()

        row = lax.broadcasted_iota(jnp.int32, (32, rows), 0)
        col = lax.broadcasted_iota(jnp.int32, (32, rows), 1)
        cols[...] = jnp.where((col & 1) == (row >> 4), col, 2 * rows)
        row2 = lax.broadcasted_iota(jnp.int32, (32, 2 * STEPS), 0)
        col2 = lax.broadcasted_iota(jnp.int32, (32, 2 * STEPS), 1)
        new_ok = jnp.logical_and((col2 & 1) == (row2 >> 4), (col2 >> 1) <= (row2 & 3))

        @pl.loop(0, count)
        def _(b):
            for off in range(GROUP):
                load(0, off, b).wait()
                load(1, off, b).wait()
            if here:
                slot = [mine ^ off for off in range(GROUP)]
                items = [packed_ref[slot[off], first + b] for off in range(GROUP)]
                bounds = [2 * pos_ref[first + b]] * GROUP
            else:
                slot = list(range(GROUP))
                items = [packed_ref[off, b] for off in range(GROUP)]
                bounds = [2 * pos_ref[(mine ^ off) * seqs + first + b] for off in range(GROUP)]
            done = attend_four(items, [k_buf[off, b] for off in range(GROUP)], [v_buf[off, b] for off in range(GROUP)], bounds, cols[...], new_ok)
            for off in range(GROUP):
                out_ref[slot[off], b] = done[off]

    any_spec = pl.BlockSpec(memory_space=pl.ANY)
    smem = pl.BlockSpec(memory_space=pltpu.SMEM)
    vmem = pl.BlockSpec(memory_space=pltpu.VMEM)
    return pl.pallas_call(
        body,
        in_specs=[smem, smem, vmem] + [any_spec] * n_in,
        out_specs=vmem,
        out_shape=jax.ShapeDtypeStruct((GROUP, count, 32, 128), jnp.bfloat16),
        scratch_shapes=[
            pltpu.VMEM((GROUP, count, rows, 128), jnp.bfloat16),
            pltpu.VMEM((GROUP, count, rows, 128), jnp.bfloat16),
            pltpu.VMEM((32, rows), jnp.int32),
            pltpu.SemaphoreType.DMA((2, GROUP, count)),
        ],
        cost_estimate=pl.CostEstimate(flops=count * 1_000_000_000, bytes_accessed=4 * count * 512 * 128 * 4, transcendentals=0),
        name="attend_here" if here else "attend_source",
    )(me, pos, packed, k_rows, v_rows, *(recvs or ()))


def spare_slot(where, i, live):
    return jnp.where(where <= live - STEPS, live + i, jnp.minimum(where + STEPS + i, live + STEPS - 1))


def cut(k_heads, v_heads, start_pos, me, first, count):
    seqs = k_heads.shape[0] // GROUP
    slots = k_heads.shape[1]
    live = slots - STEPS
    offs = (2, 3, 1)

    def body(me_ref, pos_ref, k_ref, v_ref, out2, out3, out1, buf, in_sems, out_sems):
        mine = me_ref[0]
        outs = (out2, out3, out1)

        def load(k, c, b):
            return pltpu.make_async_copy((k_ref, v_ref)[c].at[(mine ^ offs[k]) * seqs + first + b], buf.at[k, c, b], in_sems.at[k, c, b])

        def store(k, c, b):
            return pltpu.make_async_copy(buf.at[k, c, b, pl.ds(0, live)], outs[k].at[c, b], out_sems.at[k, c, b])

        for k in range(3):

            @pl.loop(0, count)
            def _(b):
                for c in range(2):
                    load(k, c, b).start()

        for k in range(3):

            @pl.loop(0, count)
            def _(b):
                where = pos_ref[(mine ^ offs[k]) * seqs + first + b]
                for c in range(2):
                    load(k, c, b).wait()
                    for i in range(STEPS):
                        buf[k, c, b, where + i] = buf[k, c, b, spare_slot(where, i, live)]
                    store(k, c, b).start()

        for k in range(3):

            @pl.loop(0, count)
            def _(b):
                for c in range(2):
                    store(k, c, b).wait()

    any_spec = pl.BlockSpec(memory_space=pl.ANY)
    smem = pl.BlockSpec(memory_space=pltpu.SMEM)
    out = pl.pallas_call(
        body,
        in_specs=[smem, smem, any_spec, any_spec],
        out_specs=[any_spec] * 3,
        out_shape=[jax.ShapeDtypeStruct((2, count, live, 2, 128), jnp.bfloat16)] * 3,
        scratch_shapes=[
            pltpu.VMEM((3, 2, count, slots, 2, 128), jnp.bfloat16),
            pltpu.SemaphoreType.DMA((3, 2, count)),
            pltpu.SemaphoreType.DMA((3, 2, count)),
        ],
        cost_estimate=pl.CostEstimate(flops=count * 600_000_000, bytes_accessed=6 * count * slots * 2 * 128 * 4, transcendentals=0),
        name="cut",
    )(me, start_pos, k_heads, v_heads)
    return dict(zip(offs, out))


def assemble(k_heads, v_heads, units, fresh, pos, me, prev):
    seqs = k_heads.shape[0] // GROUP
    slots = k_heads.shape[1]
    total = sum(count for _, count, _ in units)
    starts = [sum(count for _, count, _ in units[:u]) for u in range(len(units))]

    def body(me_ref, pos_ref, k_ref, v_ref, k_fresh, v_fresh, *rest):
        k_out, v_out, buf, fresh_buf, in_sems, fresh_sems, out_sems = rest[-7:]
        mine = me_ref[0]

        def load(u, c, b, off):
            at = starts[u] + b
            live = units[u][2][0].shape[2]
            if off == 0:
                src = (k_ref, v_ref)[c].at[mine * seqs + units[u][0] + b]
                return pltpu.make_async_copy(src, buf.at[c, at, :, mine], in_sems.at[c, at, 0])
            return pltpu.make_async_copy(rest[3 * u + off - 1].at[c, b], buf.at[c, at, pl.ds(0, live), mine ^ off], in_sems.at[c, at, off])

        def load_fresh(u, c):
            first, count, _ = units[u]
            return pltpu.make_async_copy((k_fresh, v_fresh)[c].at[pl.ds(first, count)], fresh_buf.at[c, pl.ds(starts[u], count)], fresh_sems.at[u, c])

        def store(u, c, b):
            at = starts[u] + b
            return pltpu.make_async_copy(buf.at[c, at], (k_out, v_out)[c].at[units[u][0] + b], out_sems.at[c, at])

        own = lax.broadcasted_iota(jnp.int32, (GROUP, 2, 128), 0) == mine
        for u in range(len(units)):
            for c in range(2):
                load_fresh(u, c).start()

        for u, (_, count, _) in enumerate(units):

            @pl.loop(0, count)
            def _(b):
                for c in range(2):
                    for off in range(GROUP):
                        load(u, c, b, off).start()

        for u, (first, count, recvs) in enumerate(units):
            live = recvs[0].shape[2]
            for c in range(2):
                load_fresh(u, c).wait()

            @pl.loop(0, count)
            def _(b):
                at = starts[u] + b
                where = pos_ref[first + b]
                for c in range(2):
                    for off in range(GROUP):
                        load(u, c, b, off).wait()
                    for i in range(STEPS if live < slots else 0):
                        spare = spare_slot(where, i, live)
                        moved = jnp.where(own, buf[c, at, spare], buf[c, at, where + i])

                        @pl.when(where + i < live)
                        def _():
                            buf[c, at, spare] = moved

                    for s in range(STEPS):
                        buf[c, at, where + s] = fresh_buf[c, at, s]
                    store(u, c, b).start()

        for u, (_, count, _) in enumerate(units):

            @pl.loop(0, count)
            def _(b):
                for c in range(2):
                    store(u, c, b).wait()

    any_spec = pl.BlockSpec(memory_space=pl.ANY)
    smem = pl.BlockSpec(memory_space=pltpu.SMEM)
    args = [me, pos, k_heads, v_heads, *fresh]
    for _, _, recvs in units:
        args += recvs
    aliases = {}
    if prev is not None:
        aliases = {len(args): 0, len(args) + 1: 1}
        args += prev
    return pl.pallas_call(
        body,
        in_specs=[smem, smem] + [any_spec] * (len(args) - 2),
        out_specs=[any_spec] * 2,
        out_shape=[jax.ShapeDtypeStruct((seqs, slots, GROUP, 2, 128), jnp.bfloat16)] * 2,
        scratch_shapes=[
            pltpu.VMEM((2, total, slots, GROUP, 2, 128), jnp.bfloat16),
            pltpu.VMEM((2, total, STEPS, GROUP, 2, 128), jnp.bfloat16),
            pltpu.SemaphoreType.DMA((2, total, GROUP)),
            pltpu.SemaphoreType.DMA((len(units), 2)),
            pltpu.SemaphoreType.DMA((2, total)),
        ],
        input_output_aliases=aliases,
        cost_estimate=pl.CostEstimate(flops=total * 600_000_000, bytes_accessed=2 * total * slots * 8 * 128 * 4, transcendentals=0),
        name="assemble",
    )(*args)


def solution(mesh):
    row_spec = P(None, ('dp', 'x'), None)
    cache_in = P('dp', None, 'x', None)
    cache_out = P(('dp', 'x'), None, None, None)

    def swap(arr, off):
        return lax.ppermute(arr, 'x', [(i, i ^ off) for i in range(GROUP)])

    def layer(start_pos, hidden_in, k_heads, v_heads, attn_norm, w_q, w_k, w_v, q_norm, k_norm, w_o, mlp_norm, w_gate, w_up, w_down):
        num_rows = hidden_in.shape[1]
        n_steps = hidden_in.shape[0]
        head_dim = q_norm.shape[0]
        slots = k_heads.shape[1]
        me = lax.axis_index('x')
        me_arr = me.reshape(1).astype(jnp.int32)
        my_pos = lax.dynamic_slice_in_dim(start_pos, me * num_rows, num_rows)
        k_rows = k_heads.reshape(k_heads.shape[0], slots * 2, head_dim)
        v_rows = v_heads.reshape(v_heads.shape[0], slots * 2, head_dim)

        def send_unit(u):
            first, count = UNITS[u]
            if u == 0:
                out = {}
                for off in (2, 3, 1):
                    at = ((me ^ off) * num_rows + first, 0, 0)
                    both = [swap(lax.dynamic_slice(rows, at, (count,) + rows.shape[1:]), off) for rows in (k_rows, v_rows)]
                    out[off] = both
            else:
                parts = cut(k_heads, v_heads, start_pos, me_arr, first, count)
                out = {}
                for off in (3, 2, 1):
                    out[off] = swap(parts[off], off)
            if u == 0:
                out = {off: lax.optimization_barrier(jnp.stack(both)).reshape(2, count, slots, 2, head_dim) for off, both in out.items()}
            return [out[off] for off in (1, 2, 3)]

        recvs = [send_unit(u) for u in range(len(UNITS))]

        positions = my_pos[None, :] + jnp.arange(n_steps)[:, None]
        queries, keys_new, values_new = project(hidden_in, positions, attn_norm, w_q, w_k, w_v, q_norm, k_norm)
        q_pack = queries.reshape(n_steps, num_rows, GROUP, 2, 4, head_dim).transpose(2, 1, 3, 4, 0, 5).reshape(GROUP, num_rows, 32, head_dim)
        kv_shape = (n_steps, num_rows, GROUP, 2, head_dim)
        k_pack = keys_new.reshape(kv_shape).transpose(2, 1, 0, 3, 4).reshape(GROUP, num_rows, 8, head_dim)
        v_pack = values_new.reshape(kv_shape).transpose(2, 1, 0, 3, 4).reshape(GROUP, num_rows, 8, head_dim)
        packed = jnp.concatenate([q_pack, k_pack, v_pack], axis=2)

        def owner_part(arr, off):
            return lax.dynamic_index_in_dim(arr, me ^ off, 0, keepdims=False)

        late = packed[:, EARLY:]
        by_off = [owner_part(late, 0)] + [swap(owner_part(late, off), off) for off in (1, 2, 3)]
        mixed = attend(jnp.stack(by_off), k_rows, v_rows, None, start_pos, me_arr, EARLY, num_rows - EARLY)
        back = jnp.stack([mixed[0]] + [swap(mixed[off], off) for off in (1, 2, 3)])
        here = []
        for g, (first, count) in enumerate(GROUPS):
            arrived = [r.reshape(2, count, -1, head_dim) for r in recvs[g]]
            here.append(attend(packed, k_rows, v_rows, arrived, my_pos, me_arr, first, count))
        there = jnp.stack([owner_part(back, j) for j in range(GROUP)])
        owners = jnp.concatenate(here + [there], axis=1)
        attended = owners.reshape(GROUP, num_rows, 2, 4, n_steps, head_dim).transpose(4, 1, 0, 2, 3, 5).reshape(n_steps, num_rows, -1)
        out_hidden = finish(hidden_in, attended, w_o, mlp_norm, w_gate, w_up, w_down, me_arr & 1, lambda arr: swap(arr, 1))

        k_fresh = keys_new.reshape(kv_shape).transpose(1, 0, 2, 3, 4)
        v_fresh = values_new.reshape(kv_shape).transpose(1, 0, 2, 3, 4)
        outs = None
        for some in ASSEMBLIES:
            outs = assemble(k_heads, v_heads, [(*UNITS[u], recvs[u]) for u in some], (k_fresh, v_fresh), my_pos, me_arr, outs)
        k_out, v_out = outs
        full = (num_rows, slots, 2 * GROUP, head_dim)
        return out_hidden, k_out.reshape(full), v_out.reshape(full)


    return jax.shard_map(layer, mesh=mesh, in_specs=(P('dp'), row_spec, cache_in, cache_in) + (P(),) * 11, out_specs=(row_spec, cache_out, cache_out), check_vma=False)
```
